32 devices in a mesh: chain: 8 (over y, x, core), col: 4 (over z).
Axes of the slice: x: 2, y: 2, z: 4, core: 2. Of those that a mesh axis runs over, the one named last changes fastest.
Arguments:
- rhs: bfloat16 [16, 64, 2560], P('chain', None, 'col'), may hold values from -6 to 6
- block_inverse: bfloat16 [16, 2560, 2560], P('chain', 'col'), as said below
- entry_factor: bfloat16 [16, 2560, 128], P('chain', 'col'), as said below
- exit_factor: bfloat16 [16, 2560, 128], P('chain', 'col'), as said below
- previous: bfloat16 [64, 2560], P(None, 'col'), may hold values from -6 to 6
Outputs:
- solution: float32 [16, 64, 2560], P('chain', None, 'col')
The draws below stay inside these ranges and needn't reach their ends.
Inputs may be any that keep to these rules, and one draw needn't show every extreme that they name: Every block of block_inverse equals its own transpose. `entry_factor`: entries are independent, of mean zero. `exit_factor`: entries are independent, of mean zero.
All inputs are finite; a program needn't handle non-finite values.
Results may differ from the reference program's by a relative error of at most 0.0003.
Values may be sent and summed in bfloat16 or wider, within the bound.
A program may use at most 64 MiB of HBM per device.

```python
import jax
import jax.numpy as jnp
from jax import lax

B = 2560
NX = 128
COLS = 64
INTERVALS = 16


def draw_block_inverse(key, part):

    def draw_block(interval):
        subkey = jax.random.fold_in(key, interval)
        first_key, second_key = jax.random.split(subkey)
        random_part = jax.random.normal(first_key, (B, B), jnp.float32)
        symmetric = (random_part + random_part.T) * (0.6 / (2.0 * B) ** 0.5)
        diagonal_part = jax.random.uniform(second_key, (B,), jnp.float32, 0.5, 2.0)
        return (symmetric + jnp.diag(diagonal_part)).astype(jnp.bfloat16)
    return lax.map(draw_block, jnp.arange(INTERVALS))


def draw_factor(key, spread):
    shape = (INTERVALS, B, NX)
    values = jax.random.truncated_normal(key, -3.0, 3.0, shape, jnp.float32) * (spread / 0.9866)
    return values.astype(jnp.bfloat16)


def draw_entry_factor(key, part):
    return draw_factor(jax.random.fold_in(key, 11), (NX * 5.0 / 4.0) ** (-0.5))


def draw_exit_factor(key, part):
    return draw_factor(jax.random.fold_in(key, 23), (1.0 * B) ** (-0.5))


def block_scale(rng, extent, cuts, low, high):
    def one(position, parts):
        draws = jax.random.uniform(jax.random.fold_in(jax.random.fold_in(rng, 6), position), (parts,), jnp.float32, low / len(cuts), high / len(cuts))
        return jnp.repeat(jnp.exp(draws), extent[position] // parts).reshape((-1,) + (1,) * (len(extent) - position - 1))

    factor_of = one(*cuts[0])
    for cut in cuts[1:]:
        factor_of = factor_of * one(*cut)
    return factor_of


def bell_draw(key, shape, scale, reach, cuts=(), dtype=jnp.bfloat16):
    result = scale * jax.random.normal(key, shape, jnp.float32)
    if cuts:
        result = result * block_scale(key, shape, cuts, -0.22, 0.18)
    return jnp.clip(result, -reach, reach).astype(dtype)


def setup_inputs(seed: int = 0) -> dict:
    streams_of = jax.random.split(jax.random.key(seed), 6)
    rhs = bell_draw(streams_of[0], (INTERVALS, COLS, B), 1.0, 6.0, ((0, 8), (2, 4)))
    block_inverse = draw_block_inverse(jax.random.fold_in(streams_of[5], 71), 0)
    entry_factor = draw_entry_factor(jax.random.fold_in(streams_of[5], 71), 0)
    exit_factor = draw_exit_factor(jax.random.fold_in(streams_of[5], 71), 0)
    previous = bell_draw(streams_of[4], (COLS, B), 1.0, 6.0, ((1, 4),))
    return {"rhs": rhs, "block_inverse": block_inverse, "entry_factor": entry_factor, "exit_factor": exit_factor, "previous": previous}


def reference(rhs, block_inverse, entry_factor, exit_factor, previous):
    exact = lax.Precision.HIGHEST
    total_intervals = rhs.shape[0]
    carry_state = jnp.dot(previous, exit_factor[0], preferred_element_type=jnp.float32)
    applied_list = []
    couplings = []
    for interval in range(total_intervals):
        solved = rhs[interval].astype(jnp.float32) - jnp.dot(carry_state, entry_factor[interval].astype(jnp.float32).T, precision=exact)
        solved_low = solved.astype(jnp.bfloat16)
        applied_list.append(jnp.dot(solved_low, block_inverse[interval], preferred_element_type=jnp.float32))
        if interval + 1 < total_intervals:
            following = exit_factor[interval + 1]
            couple = -jnp.dot(entry_factor[interval].T, following, preferred_element_type=jnp.float32)
            source = jnp.dot(rhs[interval], following, preferred_element_type=jnp.float32)
            carry_state = jnp.dot(carry_state, couple, precision=exact) + source
            couplings.append(couple)
    behind = jnp.zeros((rhs.shape[1], entry_factor.shape[2]), jnp.float32)
    results = [None] * total_intervals
    for interval in reversed(range(total_intervals)):
        applied = applied_list[interval]
        if interval + 1 < total_intervals:
            results[interval] = applied - jnp.dot(behind, exit_factor[interval + 1].astype(jnp.float32).T, precision=exact)
        else:
            results[interval] = applied
        if interval > 0:
            carried = jnp.dot(applied.astype(jnp.bfloat16), entry_factor[interval], preferred_element_type=jnp.float32)
            if interval + 1 < total_intervals:
                behind = jnp.dot(behind, couplings[interval].T, precision=exact) + carried
            else:
                behind = carried
    return jnp.stack(results)
```

```python
import functools

import jax
import jax.numpy as jnp
from jax import lax
from jax.experimental import pallas as pl
from jax.experimental.pallas import tpu as pltpu
from jax.sharding import PartitionSpec as P

MESH = pl.DeviceIdType.MESH
F32 = jnp.float32
BF16 = jnp.bfloat16


def dot_t(a, b):
    return lax.dot_general(a, b, (((1,), (1,)), ((), ())), preferred_element_type=F32)


def terms(x):
    first = x.astype(BF16)
    rest = x - first.astype(F32)
    second = rest.astype(BF16)
    third = (rest - second.astype(F32)).astype(BF16)
    return first, second, third


def split_dot_t(x, low):
    rows = x.shape[0]
    product = dot_t(jnp.concatenate(terms(x), axis=0), low)
    return (product[2 * rows:] + product[rows:2 * rows]) + product[:rows]


def wide_dot(a, b, dot):
    rows = a.shape[0]
    a1, a2, a3 = terms(a)
    b1, b2, b3 = terms(b)
    p1 = dot(jnp.concatenate([a1, a2, a3], axis=0), b1)
    p2 = dot(jnp.concatenate([a1, a2], axis=0), b2)
    p3 = dot(a1, b3)
    small = (p1[2 * rows:] + p2[rows:]) + p3
    return (small + (p1[rows:2 * rows] + p2[:rows])) + p1[:rows]


def plain_dot(a, b):
    return jnp.dot(a, b, preferred_element_type=F32)


def exact_dot(a, b):
    return wide_dot(a, b, plain_dot)


def exact_dot_t(a, b):
    return wide_dot(a, b, dot_t)


def kernel(
    n, m, rhs_hbm, binv_hbm, entry_hbm, exit_hbm, prev_hbm, out_ref,
    rhs, binv, entry, exits, prev, arriving,
    parts, parts_in, opening, opening_in, summed, comp, gathered,
    states, forward, applied, carried, carried_in, carried_sum, back, back_in, behind,
    local_sem, exit_sem, part_send, part_recv, open_send, open_recv,
    comp_send, comp_recv, state_send, state_recv, fwd_send, fwd_recv,
    car_send, car_recv, back_send, back_recv, beh_send, beh_recv,
):
    c = lax.axis_index("chain")
    k = lax.axis_index("col")
    count, columns, width = rhs.shape
    nx = entry.shape[2]

    def owner_of(chain):
        return m // 2 - 1 + lax.rem(chain, 2)

    owner = owner_of(c)
    is_owner = k == owner
    unsent = []

    def remote(src, dst, send, recv, where):
        return pltpu.make_async_remote_copy(
            src_ref=src, dst_ref=dst, send_sem=send, recv_sem=recv,
            device_id=where, device_id_type=MESH,
        )

    def send(condition, *args):
        @pl.when(condition)
        def _():
            remote(*args).start()

        unsent.append((condition, args))

    loads = [
        pltpu.make_async_copy(exit_hbm, exits, local_sem.at[0]),
        pltpu.make_async_copy(entry_hbm, entry, local_sem.at[1]),
        pltpu.make_async_copy(rhs_hbm, rhs, local_sem.at[2]),
        pltpu.make_async_copy(prev_hbm, prev, local_sem.at[3]),
    ] + [
        pltpu.make_async_copy(binv_hbm.at[p], binv.at[p], local_sem.at[4 + p])
        for p in range(count)
    ]
    for load in loads:
        load.start()

    barrier = pltpu.get_barrier_semaphore()
    for d in range(1, m):
        pl.semaphore_signal(
            barrier, 1, device_id={"col": lax.rem(k + d, m)}, device_id_type=MESH
        )

    @pl.when(c > 0)
    def _():
        pl.semaphore_signal(barrier, 1, device_id={"chain": c - 1}, device_id_type=MESH)

    @pl.when(c < n - 1)
    def _():
        pl.semaphore_signal(barrier, 1, device_id={"chain": c + 1}, device_id_type=MESH)

    @pl.when(is_owner)
    def _():
        for d in range(1, n):
            other = lax.rem(c + d, n)
            pl.semaphore_signal(
                barrier, 1, device_id={"chain": other, "col": owner_of(other)},
                device_id_type=MESH,
            )

    @pl.when(c == n - 1)
    def _():
        arriving[...] = jnp.zeros_like(arriving)

    expected = m - 1 + jnp.where(c > 0, 1, 0) + jnp.where(c < n - 1, 1, 0)
    pl.semaphore_wait(barrier, expected + jnp.where(is_owner, n - 1, 0))

    loads[0].wait()
    send(c > 0, exits.at[0], arriving, exit_sem.at[0], exit_sem.at[1], {"chain": c - 1})
    for load in loads[1:4]:
        load.wait()

    @pl.when(c == 0)
    def _():
        opening[...] = jnp.dot(prev[...], exits[0], preferred_element_type=F32)

    send(
        (c == 0) & jnp.logical_not(is_owner), opening, opening_in.at[k],
        open_send, open_recv.at[k], {"col": owner},
    )

    def following(p):
        return exits[p + 1] if p + 1 < count else arriving[...]

    for p in range(count):
        if p + 1 == count:
            @pl.when(c < n - 1)
            def _():
                remote(
                    exits.at[0], arriving, exit_sem.at[0], exit_sem.at[1], {"chain": c}
                ).wait_recv()
        parts[p, :nx] = -lax.dot_general(
            entry[p], following(p), (((0,), (0,)), ((), ())), preferred_element_type=F32
        )
        parts[p, nx:] = jnp.dot(rhs[p], following(p), preferred_element_type=F32)
        send(
            jnp.logical_not(is_owner), parts.at[p], parts_in.at[k, p],
            part_send.at[p], part_recv.at[k, p], {"col": owner},
        )

    def spread(buffer, p, sends, recvs):
        for d in range(1, m):
            send(
                is_owner, buffer.at[p], buffer.at[p], sends.at[p, d - 1], recvs.at[p],
                {"col": lax.rem(k + d, m)},
            )

    @pl.when(is_owner)
    def _():
        for p in range(count):
            for d in range(1, m):
                other = lax.rem(k + d, m)
                remote(
                    parts.at[p], parts_in.at[other, p], part_send.at[p],
                    part_recv.at[other, p], {"col": other},
                ).wait_recv()
            total = parts[p]
            for d in range(1, m):
                total += parts_in[lax.rem(k + d, m), p]
            summed[p] = total
        both = summed[0]
        for p in range(1, count):
            both = exact_dot(both, summed[p, :nx])
            both = jnp.concatenate([both[:nx], both[nx:] + summed[p, nx:]], axis=0)
        comp[...] = both

        @pl.when(c == 0)
        def _():
            total = opening[...]
            for d in range(1, m):
                other = lax.rem(k + d, m)
                remote(
                    opening, opening_in.at[other], open_send,
                    open_recv.at[other], {"col": other},
                ).wait_recv()
                total += opening_in[other]
            states[0] = total
            comp[nx:] = exact_dot(total, comp[:nx]) + comp[nx:]

    for d in range(1, n):
        later = lax.rem(c + d, n)
        send(
            is_owner & (c + d < n), comp, gathered.at[c], comp_send.at[d - 1],
            comp_recv.at[c], {"chain": later, "col": owner_of(later)},
        )
    for d in range(1, n):
        earlier = lax.rem(c - d + n, n)
        send(
            is_owner & (c - d >= 0), comp.at[pl.ds(0, nx)], gathered.at[c, pl.ds(0, nx)],
            comp_send.at[n - 1 + d - 1], comp_recv.at[c],
            {"chain": earlier, "col": owner_of(earlier)},
        )

    @pl.when(is_owner & (c > 0))
    def _():
        def fold(s, state):
            remote(
                comp, gathered.at[s], comp_send.at[0], comp_recv.at[s], {"chain": c}
            ).wait_recv()
            return exact_dot(state, gathered[s, :nx]) + gathered[s, nx:]

        states[0] = lax.fori_loop(0, c, fold, jnp.zeros((columns, nx), F32))

    for p in range(count):
        if p > 0:
            @pl.when(is_owner)
            def _():
                states[p] = exact_dot(states[p - 1], summed[p - 1, :nx]) + summed[p - 1, nx:]
        spread(states, p, state_send, state_recv)

    for p in range(count):
        @pl.when(jnp.logical_not(is_owner))
        def _():
            remote(
                states.at[p], states.at[p], state_send.at[p, 0], state_recv.at[p], {"col": k}
            ).wait_recv()
        forward[k, p] = (
            rhs[p].astype(F32) - split_dot_t(states[p], entry[p])
        ).astype(BF16)
        for way, step in ((0, 1), (1, -1)):
            beyond = k + step
            send(
                (beyond >= 0) & (beyond < m), forward.at[k, p], forward.at[k, p],
                fwd_send.at[k, p, way], fwd_recv.at[k, p], {"col": beyond},
            )

    def block(j, p):
        return binv[p, :, pl.ds(pl.multiple_of(j * width, 128), width)]

    for p in range(count):
        loads[4 + p].wait()
        applied[p] = dot_t(forward[k, p], block(k, p))
    for d in range(1, m):
        for p in range(count):
            for way, step in ((0, 1), (1, -1)):
                j = k - step * d
                beyond = k + step
                there = (j >= 0) & (j < m)

                @pl.when(there)
                def _():
                    remote(
                        forward.at[j, p], forward.at[j, p], fwd_send.at[j, p, way],
                        fwd_recv.at[j, p], {"col": j},
                    ).wait_recv()

                send(
                    there & (beyond >= 0) & (beyond < m), forward.at[j, p], forward.at[j, p],
                    fwd_send.at[j, p, way], fwd_recv.at[j, p], {"col": beyond},
                )

                @pl.when(there)
                def _():
                    applied[p] += dot_t(forward[j, p], block(j, p))

    for p in reversed(range(count)):
        carried[p] = jnp.dot(applied[p].astype(BF16), entry[p], preferred_element_type=F32)
        send(
            jnp.logical_not(is_owner), carried.at[p], carried_in.at[k, p],
            car_send.at[p], car_recv.at[k, p], {"col": owner},
        )

    @pl.when(is_owner)
    def _():
        offset = None
        for p in reversed(range(count)):
            total = carried[p]
            for d in range(1, m):
                other = lax.rem(k + d, m)
                remote(
                    carried.at[p], carried_in.at[other, p], car_send.at[p],
                    car_recv.at[other, p], {"col": other},
                ).wait_recv()
                total += carried_in[other, p]
            carried_sum[p] = total
            if offset is None:
                offset = total
            else:
                offset = exact_dot_t(offset, summed[p, :nx]) + total
        back[...] = offset

    for d in range(1, n):
        earlier = lax.rem(c - d + n, n)
        send(
            is_owner & (c - d >= 0), back, back_in.at[c], back_send.at[d - 1],
            back_recv.at[c], {"chain": earlier, "col": owner_of(earlier)},
        )

    @pl.when(is_owner)
    def _():
        def fold(i, state):
            s = n - 1 - i
            remote(
                comp.at[pl.ds(0, nx)], gathered.at[s, pl.ds(0, nx)], comp_send.at[0],
                comp_recv.at[s], {"chain": c},
            ).wait_recv()
            remote(
                back, back_in.at[s], back_send.at[0], back_recv.at[s], {"chain": c}
            ).wait_recv()
            return exact_dot_t(state, gathered[s, :nx]) + back_in[s]

        behind[count - 1] = lax.fori_loop(0, n - 1 - c, fold, jnp.zeros((columns, nx), F32))

    for p in reversed(range(count)):
        if p + 1 < count:
            @pl.when(is_owner)
            def _():
                behind[p] = exact_dot_t(behind[p + 1], summed[p + 1, :nx]) + carried_sum[p + 1]
        spread(behind, p, beh_send, beh_recv)

    for p in reversed(range(count)):
        @pl.when(jnp.logical_not(is_owner))
        def _():
            remote(
                behind.at[p], behind.at[p], beh_send.at[p, 0], beh_recv.at[p], {"col": k}
            ).wait_recv()
        out_ref[p] = applied[p] - split_dot_t(behind[p], following(p))

    for condition, args in unsent:
        @pl.when(condition)
        def _():
            remote(*args).wait_send()


def shards(n, m, rhs, block_inverse, entry_factor, exit_factor, previous):
    count, columns, width = rhs.shape
    nx = entry_factor.shape[2]
    padded = -(-width // 128) * 128
    if padded != width:
        extra = padded - width
        rhs = jnp.pad(rhs, ((0, 0), (0, 0), (0, extra)))
        previous = jnp.pad(previous, ((0, 0), (0, extra)))
        entry_factor = jnp.pad(entry_factor, ((0, 0), (0, extra), (0, 0)))
        exit_factor = jnp.pad(exit_factor, ((0, 0), (0, extra), (0, 0)))
        block_inverse = jnp.pad(
            block_inverse.reshape(count, width, m, width),
            ((0, 0), (0, extra), (0, 0), (0, extra)),
        ).reshape(count, padded, m * padded)
    vmem = pltpu.VMEM
    dma = pltpu.SemaphoreType.DMA
    out = pl.pallas_call(
        functools.partial(kernel, n, m),
        out_shape=jax.ShapeDtypeStruct((count, columns, padded), F32),
        in_specs=[pl.BlockSpec(memory_space=pl.ANY)] * 5,
        out_specs=pl.BlockSpec(memory_space=pltpu.VMEM),
        scratch_shapes=[
            vmem((count, columns, padded), BF16),
            vmem(block_inverse.shape, BF16),
            vmem(entry_factor.shape, BF16),
            vmem(exit_factor.shape, BF16),
            vmem(previous.shape, BF16),
            vmem(exit_factor.shape[1:], BF16),
            vmem((count, nx + columns, nx), F32),
            vmem((m, count, nx + columns, nx), F32),
            vmem((columns, nx), F32),
            vmem((m, columns, nx), F32),
            vmem((count, nx + columns, nx), F32),
            vmem((nx + columns, nx), F32),
            vmem((n, nx + columns, nx), F32),
            vmem((count, columns, nx), F32),
            vmem((m, count, columns, padded), BF16),
            vmem((count, columns, padded), F32),
            vmem((count, columns, nx), F32),
            vmem((m, count, columns, nx), F32),
            vmem((count, columns, nx), F32),
            vmem((columns, nx), F32),
            vmem((n, columns, nx), F32),
            vmem((count, columns, nx), F32),
            dma((4 + count,)),
            dma((2,)),
            dma((count,)), dma((m, count)),
            dma(()), dma((m,)),
            dma((2 * (n - 1),)), dma((n,)),
            dma((count, m - 1)), dma((count,)),
            dma((m, count, 2)), dma((m, count)),
            dma((count,)), dma((m, count)),
            dma((n - 1,)), dma((n,)),
            dma((count, m - 1)), dma((count,)),
        ],
        compiler_params=pltpu.CompilerParams(
            collective_id=0, has_side_effects=True, vmem_limit_bytes=48 * 1024 * 1024
        ),
    )(rhs, block_inverse, entry_factor, exit_factor, previous)
    return out[:, :, :width] if padded != width else out


def solution(mesh):
    placed = (
        P("chain", None, "col"),
        P("chain", "col", None),
        P("chain", "col", None),
        P("chain", "col", None),
        P(None, "col"),
    )
    return jax.shard_map(
        functools.partial(shards, mesh.shape["chain"], mesh.shape["col"]),
        mesh=mesh, in_specs=placed, out_specs=P("chain", None, "col"), check_vma=False,
    )
```

```python
import functools

import jax
import jax.numpy as jnp
from jax import lax
from jax.experimental import pallas as pl
from jax.experimental.pallas import tpu as pltpu
from jax.sharding import PartitionSpec as P

MESH = pl.DeviceIdType.MESH
F32 = jnp.float32
BF16 = jnp.bfloat16


def dot_t(a, b):
    return lax.dot_general(a, b, (((1,), (1,)), ((), ())), preferred_element_type=F32)


def terms(x):
    first = x.astype(BF16)
    rest = x - first.astype(F32)
    second = rest.astype(BF16)
    third = (rest - second.astype(F32)).astype(BF16)
    return first, second, third


def split_dot_t(x, low):
    rows = x.shape[0]
    product = dot_t(jnp.concatenate(terms(x), axis=0), low)
    return (product[2 * rows:] + product[rows:2 * rows]) + product[:rows]


def exact_dot(a, b):
    a1, a2, a3 = terms(a)
    b1, b2, b3 = terms(b)
    return jnp.dot(
        jnp.concatenate([a3, a2, a1, a2, a1, a1], axis=1),
        jnp.concatenate([b1, b2, b3, b1, b2, b1], axis=0),
        preferred_element_type=F32,
    )


def exact_dot_t(a, b):
    a1, a2, a3 = terms(a)
    b1, b2, b3 = terms(b)
    return dot_t(
        jnp.concatenate([a3, a2, a1, a2, a1, a1], axis=1),
        jnp.concatenate([b1, b2, b3, b1, b2, b1], axis=1),
    )


def kernel(
    n, m, rhs_hbm, binv_hbm, entry_hbm, exit_hbm, prev_hbm, out_ref,
    rhs, binv, entry, exits, prev, arriving,
    parts, parts_in, opening, opening_in, summed, comp, gathered,
    states, forward, applied, carried, carried_in, carried_sum, back, back_in, behind,
    local_sem, exit_sem, part_send, part_recv, open_send, open_recv,
    comp_send, comp_recv, state_send, state_recv, fwd_send, fwd_recv,
    car_send, car_recv, back_send, back_recv, beh_send, beh_recv,
):
    c = lax.axis_index("chain")
    k = lax.axis_index("col")
    count, columns, width = rhs.shape
    nx = entry.shape[2]

    def owner_of(chain):
        return m // 2 - 1 + lax.rem(chain, 2)

    owner = owner_of(c)
    is_owner = k == owner
    unsent = []

    def remote(src, dst, send, recv, where):
        return pltpu.make_async_remote_copy(
            src_ref=src, dst_ref=dst, send_sem=send, recv_sem=recv,
            device_id=where, device_id_type=MESH,
        )

    def send(condition, *args):
        @pl.when(condition)
        def _():
            remote(*args).start()

        unsent.append((condition, args))

    loads = [
        pltpu.make_async_copy(exit_hbm, exits, local_sem.at[0]),
        pltpu.make_async_copy(entry_hbm, entry, local_sem.at[1]),
        pltpu.make_async_copy(rhs_hbm, rhs, local_sem.at[2]),
        pltpu.make_async_copy(prev_hbm, prev, local_sem.at[3]),
    ] + [
        pltpu.make_async_copy(binv_hbm.at[p], binv.at[p], local_sem.at[4 + p])
        for p in range(count)
    ]
    for load in loads:
        load.start()

    barrier = pltpu.get_barrier_semaphore()
    for d in range(1, m):
        pl.semaphore_signal(
            barrier, 1, device_id={"col": lax.rem(k + d, m)}, device_id_type=MESH
        )

    @pl.when(c > 0)
    def _():
        pl.semaphore_signal(barrier, 1, device_id={"chain": c - 1}, device_id_type=MESH)

    @pl.when(c < n - 1)
    def _():
        pl.semaphore_signal(barrier, 1, device_id={"chain": c + 1}, device_id_type=MESH)

    @pl.when(is_owner)
    def _():
        for d in range(1, n):
            other = lax.rem(c + d, n)
            pl.semaphore_signal(
                barrier, 1, device_id={"chain": other, "col": owner_of(other)},
                device_id_type=MESH,
            )

    @pl.when(c == n - 1)
    def _():
        arriving[...] = jnp.zeros_like(arriving)

    for load in loads[:4]:
        load.wait()

    @pl.when(c == 0)
    def _():
        opening[...] = jnp.dot(prev[...], exits[0], preferred_element_type=F32)

    def following(p):
        return exits[p + 1] if p + 1 < count else arriving[...]

    def part(p):
        parts[p, :nx] = -lax.dot_general(
            entry[p], following(p), (((0,), (0,)), ((), ())), preferred_element_type=F32
        )
        parts[p, nx:] = jnp.dot(rhs[p], following(p), preferred_element_type=F32)

    for p in range(count - 1):
        part(p)

    expected = m - 1 + jnp.where(c > 0, 1, 0) + jnp.where(c < n - 1, 1, 0)
    pl.semaphore_wait(barrier, expected + jnp.where(is_owner, n - 1, 0))

    send(c > 0, exits.at[0], arriving, exit_sem.at[0], exit_sem.at[1], {"chain": c - 1})
    send(
        (c == 0) & jnp.logical_not(is_owner), opening, opening_in.at[k],
        open_send, open_recv.at[k], {"col": owner},
    )

    for p in range(count):
        if p + 1 == count:
            @pl.when(c < n - 1)
            def _():
                remote(
                    exits.at[0], arriving, exit_sem.at[0], exit_sem.at[1], {"chain": c}
                ).wait_recv()
            part(p)
        send(
            jnp.logical_not(is_owner), parts.at[p], parts_in.at[k, p],
            part_send.at[p], part_recv.at[k, p], {"col": owner},
        )

    def spread(buffer, p, sends, recvs):
        for d in range(1, m):
            send(
                is_owner, buffer.at[p], buffer.at[p], sends.at[p, d - 1], recvs.at[p],
                {"col": lax.rem(k + d, m)},
            )

    @pl.when(is_owner)
    def _():
        for p in range(count):
            for d in range(1, m):
                other = lax.rem(k + d, m)
                remote(
                    parts.at[p], parts_in.at[other, p], part_send.at[p],
                    part_recv.at[other, p], {"col": other},
                ).wait_recv()
            total = parts[p]
            for d in range(1, m):
                total += parts_in[lax.rem(k + d, m), p]
            summed[p] = total
        both = summed[0]
        for p in range(1, count):
            both = exact_dot(both, summed[p, :nx])
            both = jnp.concatenate([both[:nx], both[nx:] + summed[p, nx:]], axis=0)
        comp[...] = both

        @pl.when(c == 0)
        def _():
            total = opening[...]
            for d in range(1, m):
                other = lax.rem(k + d, m)
                remote(
                    opening, opening_in.at[other], open_send,
                    open_recv.at[other], {"col": other},
                ).wait_recv()
                total += opening_in[other]
            states[0] = total
            comp[nx:] = exact_dot(total, comp[:nx]) + comp[nx:]

    for d in range(1, n):
        later = lax.rem(c + d, n)
        there = {"chain": later, "col": owner_of(later)}
        send(
            is_owner & (c > 0) & (c + d < n), comp, gathered.at[c], comp_send.at[d - 1],
            comp_recv.at[c], there,
        )
        send(
            is_owner & (c == 0), comp.at[pl.ds(nx, columns)],
            gathered.at[c, pl.ds(nx, columns)], comp_send.at[d - 1], comp_recv.at[c], there,
        )
    for d in range(1, n):
        earlier = lax.rem(c - d + n, n)
        send(
            is_owner & (c - d >= 0), comp.at[pl.ds(0, nx)], gathered.at[c, pl.ds(0, nx)],
            comp_send.at[n - 1 + d - 1], comp_recv.at[c],
            {"chain": earlier, "col": owner_of(earlier)},
        )

    @pl.when(is_owner & (c > 0))
    def _():
        def fold(s, state):
            remote(
                comp, gathered.at[s], comp_send.at[0], comp_recv.at[s], {"chain": c}
            ).wait_recv()
            return exact_dot(state, gathered[s, :nx]) + gathered[s, nx:]

        remote(
            comp.at[pl.ds(nx, columns)], gathered.at[0, pl.ds(nx, columns)],
            comp_send.at[0], comp_recv.at[0], {"chain": c},
        ).wait_recv()
        states[0] = lax.fori_loop(1, c, fold, gathered[0, nx:])

    for p in range(count):
        if p > 0:
            @pl.when(is_owner)
            def _():
                states[p] = exact_dot(states[p - 1], summed[p - 1, :nx]) + summed[p - 1, nx:]
        spread(states, p, state_send, state_recv)

    for p in range(count):
        @pl.when(jnp.logical_not(is_owner))
        def _():
            remote(
                states.at[p], states.at[p], state_send.at[p, 0], state_recv.at[p], {"col": k}
            ).wait_recv()
        forward[k, p] = (
            rhs[p].astype(F32) - split_dot_t(states[p], entry[p])
        ).astype(BF16)
        for way, step in ((0, 1), (1, -1)):
            beyond = k + step
            send(
                (beyond >= 0) & (beyond < m), forward.at[k, p], forward.at[k, p],
                fwd_send.at[k, p, way], fwd_recv.at[k, p], {"col": beyond},
            )

    def block(j, p):
        return binv[p, :, pl.ds(pl.multiple_of(j * width, 128), width)]

    for p in range(count):
        loads[4 + p].wait()
        applied[p] = dot_t(forward[k, p], block(k, p))
    for d in range(1, m):
        for p in range(count):
            for way, step in ((0, 1), (1, -1)):
                j = k - step * d
                beyond = k + step
                there = (j >= 0) & (j < m)

                @pl.when(there)
                def _():
                    remote(
                        forward.at[j, p], forward.at[j, p], fwd_send.at[j, p, way],
                        fwd_recv.at[j, p], {"col": j},
                    ).wait_recv()

                send(
                    there & (beyond >= 0) & (beyond < m),
                    forward.at[j, p], forward.at[j, p],
                    fwd_send.at[j, p, way], fwd_recv.at[j, p], {"col": beyond},
                )
            for step in (1, -1):
                j = k - step * d

                @pl.when((j >= 0) & (j < m))
                def _():
                    applied[p] += dot_t(forward[j, p], block(j, p))
            if d == m - 1:
                carried[p] = jnp.dot(
                    applied[p].astype(BF16), entry[p], preferred_element_type=F32
                )
                send(
                    jnp.logical_not(is_owner), carried.at[p], carried_in.at[k, p],
                    car_send.at[p], car_recv.at[k, p], {"col": owner},
                )

    @pl.when(is_owner)
    def _():
        offset = None
        for p in reversed(range(count)):
            total = carried[p]
            for d in range(1, m):
                other = lax.rem(k + d, m)
                remote(
                    carried.at[p], carried_in.at[other, p], car_send.at[p],
                    car_recv.at[other, p], {"col": other},
                ).wait_recv()
                total += carried_in[other, p]
            carried_sum[p] = total
            if offset is None:
                offset = total
            else:
                offset = exact_dot_t(offset, summed[p, :nx]) + total
        back[...] = offset

    for d in range(1, n):
        earlier = lax.rem(c - d + n, n)
        send(
            is_owner & (c - d >= 0), back, back_in.at[c], back_send.at[d - 1],
            back_recv.at[c], {"chain": earlier, "col": owner_of(earlier)},
        )

    @pl.when(is_owner)
    def _():
        def fold(i, state):
            s = n - 1 - i
            remote(
                comp.at[pl.ds(0, nx)], gathered.at[s, pl.ds(0, nx)], comp_send.at[0],
                comp_recv.at[s], {"chain": c},
            ).wait_recv()
            remote(
                back, back_in.at[s], back_send.at[0], back_recv.at[s], {"chain": c}
            ).wait_recv()
            return exact_dot_t(state, gathered[s, :nx]) + back_in[s]

        behind[count - 1] = lax.fori_loop(0, n - 1 - c, fold, jnp.zeros((columns, nx), F32))

    for p in reversed(range(count)):
        if p + 1 < count:
            @pl.when(is_owner)
            def _():
                behind[p] = exact_dot_t(behind[p + 1], summed[p + 1, :nx]) + carried_sum[p + 1]
        spread(behind, p, beh_send, beh_recv)

    for p in reversed(range(count)):
        @pl.when(jnp.logical_not(is_owner))
        def _():
            remote(
                behind.at[p], behind.at[p], beh_send.at[p, 0], beh_recv.at[p], {"col": k}
            ).wait_recv()
        out_ref[p] = applied[p] - split_dot_t(behind[p], following(p))

    for condition, args in unsent:
        @pl.when(condition)
        def _():
            remote(*args).wait_send()


def shards(n, m, rhs, block_inverse, entry_factor, exit_factor, previous):
    count, columns, width = rhs.shape
    nx = entry_factor.shape[2]
    padded = -(-width // 128) * 128
    if padded != width:
        extra = padded - width
        rhs = jnp.pad(rhs, ((0, 0), (0, 0), (0, extra)))
        previous = jnp.pad(previous, ((0, 0), (0, extra)))
        entry_factor = jnp.pad(entry_factor, ((0, 0), (0, extra), (0, 0)))
        exit_factor = jnp.pad(exit_factor, ((0, 0), (0, extra), (0, 0)))
        block_inverse = jnp.pad(
            block_inverse.reshape(count, width, m, width),
            ((0, 0), (0, extra), (0, 0), (0, extra)),
        ).reshape(count, padded, m * padded)
    vmem = pltpu.VMEM
    dma = pltpu.SemaphoreType.DMA
    out = pl.pallas_call(
        functools.partial(kernel, n, m),
        out_shape=jax.ShapeDtypeStruct((count, columns, padded), F32),
        in_specs=[pl.BlockSpec(memory_space=pl.ANY)] * 5,
        out_specs=pl.BlockSpec(memory_space=pltpu.VMEM),
        scratch_shapes=[
            vmem((count, columns, padded), BF16),
            vmem(block_inverse.shape, BF16),
            vmem(entry_factor.shape, BF16),
            vmem(exit_factor.shape, BF16),
            vmem(previous.shape, BF16),
            vmem(exit_factor.shape[1:], BF16),
            vmem((count, nx + columns, nx), F32),
            vmem((m, count, nx + columns, nx), F32),
            vmem((columns, nx), F32),
            vmem((m, columns, nx), F32),
            vmem((count, nx + columns, nx), F32),
            vmem((nx + columns, nx), F32),
            vmem((n, nx + columns, nx), F32),
            vmem((count, columns, nx), F32),
            vmem((m, count, columns, padded), BF16),
            vmem((count, columns, padded), F32),
            vmem((count, columns, nx), F32),
            vmem((m, count, columns, nx), F32),
            vmem((count, columns, nx), F32),
            vmem((columns, nx), F32),
            vmem((n, columns, nx), F32),
            vmem((count, columns, nx), F32),
            dma((4 + count,)),
            dma((2,)),
            dma((count,)), dma((m, count)),
            dma(()), dma((m,)),
            dma((2 * (n - 1),)), dma((n,)),
            dma((count, m - 1)), dma((count,)),
            dma((m, count, 2)), dma((m, count)),
            dma((count,)), dma((m, count)),
            dma((n - 1,)), dma((n,)),
            dma((count, m - 1)), dma((count,)),
        ],
        compiler_params=pltpu.CompilerParams(
            collective_id=0, has_side_effects=True
        ),
    )(rhs, block_inverse, entry_factor, exit_factor, previous)
    return out[:, :, :width] if padded != width else out


def solution(mesh):
    placed = (
        P("chain", None, "col"),
        P("chain", "col", None),
        P("chain", "col", None),
        P("chain", "col", None),
        P(None, "col"),
    )
    return jax.shard_map(
        functools.partial(shards, mesh.shape["chain"], mesh.shape["col"]),
        mesh=mesh, in_specs=placed, out_specs=P("chain", None, "col"), check_vma=False,
    )
```
